32 devices in a mesh: dp: 8 (over z, y), mp: 4 (over x, core).
Axes of the slice: x: 2, y: 2, z: 4, core: 2. Of those that a mesh axis runs over, the one named last changes fastest.
Arguments:
- hidden: bfloat16 [5632, 7168], P('dp', 'mp'), may hold values from -0.1875 to 0.1875
- router_weight: bfloat16 [7168, 256], P(('mp', 'dp')), may hold values from -3 to 3
- logits: float32 [5632, 256], P(('dp', 'mp')), may hold values from -12 to 240
- first_pot: float32 [256], replicated, may hold values from -1 to 1
- second_pot: float32 [256], replicated, may hold values from -1 to 1
- expert_index: int32 [5632], P(('dp', 'mp')), may hold values from 0 to 255
- loss_grad: float32 [5632], P(('dp', 'mp')), may hold values from -9 to 9
Outputs:
- weight_grad: float32 [7168, 256], P(('mp', 'dp'))
- hidden_grad: bfloat16 [5632, 7168], P('dp', 'mp')
The draws below stay inside these ranges and needn't reach their ends.
All inputs are finite; a program needn't handle non-finite values.
Results may differ from the reference program's by a relative error of at most 0.005.
Values may be sent and summed in bfloat16 or wider, within the bound.
A program may use at most 64 MiB of HBM per device.

```python
import jax
import jax.numpy as jnp
from jax import lax

D = 7168
E = 256
TOK_DEV = 704
TOKENS = 5632


def draw_logits(key, part):
    second_key = jax.random.fold_in(jax.random.fold_in(key, 11), 1)
    base = jax.random.normal(second_key, (TOKENS, E), jnp.float32) * 2.0
    return jnp.clip(base, -8.0, 8.0)


def draw_loss_grad(key, part):
    first_key, second_key, third_key = jax.random.split(jax.random.fold_in(key, 23), 3)
    blocks = TOKENS // TOK_DEV
    scales = jnp.exp(jax.random.uniform(first_key, (blocks, 1), jnp.float32, -3.0, 1.0986))
    common_sign = jnp.where(jax.random.bernoulli(second_key, 0.5, ()), 1.0, -1.0)
    noise = jnp.clip(jax.random.normal(third_key, (blocks, TOK_DEV), jnp.float32) * 0.5, -2.0, 2.0)
    return (scales * (0.7 * common_sign + noise)).reshape(TOKENS)


def with_ends(array, stream_key, smallest, high):
    longest = array.shape.index(max(array.shape))
    spots = []
    for shift in (0, 1):
        where = [jax.random.randint(jax.random.fold_in(stream_key, axis), (), 0, length) for axis, length in enumerate(array.shape)]
        where[longest] = (where[longest] + shift) % array.shape[longest]
        spots.append(tuple(where))
    return array.at[spots[0]].set(smallest).at[spots[1]].set(high)


def level_of(rng, dims, pieces, least, high):
    def one(dim, parts):
        steps = jax.random.uniform(jax.random.fold_in(jax.random.fold_in(rng, 6), dim), (parts,), jnp.float32, least / len(pieces), high / len(pieces))
        return jnp.repeat(jnp.exp(steps), dims[dim] // parts).reshape((-1,) + (1,) * (len(dims) - dim - 1))

    gain = one(*pieces[0])
    for cut in pieces[1:]:
        gain = gain * one(*cut)
    return gain


def centred(key, shape, width, limit, cuts=(), kind=jnp.bfloat16):
    level = level_of(key, shape, cuts, -0.22, 0.18) if cuts else 1.0
    drawn = jax.random.normal(key, shape, jnp.float32) * width * level
    return jnp.minimum(jnp.maximum(drawn, -limit), limit).astype(kind)


def setup_inputs(seed: int = 0) -> dict:
    seeds = jax.random.split(jax.random.key(seed), 8)
    return {
        "hidden": centred(seeds[0], (TOKENS, D), 0.03, 0.1875, ((0, 8), (1, 4))),
        "router_weight": centred(seeds[1], (D, E), 0.5, 3.0, ((0, 32),)),
        "logits": draw_logits(jax.random.fold_in(seeds[7], 71), 0),
        "first_pot": jnp.clip(jax.random.uniform(seeds[3], (E,), jnp.float32, -1.0, 1.0), -1.0, 1.0),
        "second_pot": jnp.clip(jax.random.uniform(seeds[4], (E,), jnp.float32, -1.0, 1.0), -1.0, 1.0),
        "expert_index": with_ends(jax.random.randint(seeds[5], (TOKENS,), 0, E), jax.random.fold_in(seeds[5], 1), 0, E - 1).astype(jnp.int32),
        "loss_grad": draw_loss_grad(jax.random.fold_in(seeds[7], 71), 0),
    }


def neg_lse(values):
    top = jnp.max(values, axis=1, keepdims=True)
    return -(top[:, 0] + jnp.log(jnp.sum(jnp.exp(values - top), axis=1)))


def reference(hidden, router_weight, logits, first_pot, second_pot, expert_index, loss_grad):
    ratio = E / TOKENS
    first_row = neg_lse(logits)
    first_soft = jnp.exp(logits + first_row[:, None])
    shifted = logits + first_pot[None, :]
    second_row = neg_lse(shifted)
    second_soft = jnp.exp(shifted + second_row[:, None])
    first_col = ratio * jnp.exp(logits + first_row[:, None] + first_pot[None, :])
    prob = jnp.exp(logits + second_row[:, None] + second_pot[None, :])
    second_col = ratio * prob
    onehot = (expert_index[:, None] == jnp.arange(E, dtype=jnp.int32)[None, :]).astype(jnp.float32)
    direct = onehot * prob * loss_grad[:, None]
    second_colgrad = jnp.sum(direct, axis=0)
    second_rowgrad = jnp.sum(direct, axis=1) - jnp.dot(second_col, second_colgrad, precision=lax.Precision.HIGHEST)
    first_colgrad = -jnp.sum(second_rowgrad[:, None] * second_soft, axis=0)
    first_rowgrad = -jnp.dot(first_col, first_colgrad, precision=lax.Precision.HIGHEST)
    score_grad = (direct - second_colgrad[None, :] * second_col - second_rowgrad[:, None] * second_soft
                  - first_colgrad[None, :] * first_col - first_rowgrad[:, None] * first_soft).astype(jnp.bfloat16)
    weight_grad = jnp.dot(hidden.T, score_grad, preferred_element_type=jnp.float32)
    hidden_grad = jnp.dot(score_grad, router_weight.T, preferred_element_type=jnp.float32).astype(jnp.bfloat16)
    return weight_grad, hidden_grad
```

```python
import functools

import jax
import jax.numpy as jnp
from jax import lax
from jax.experimental import pallas as pl
from jax.experimental.pallas import tpu as pltpu
from jax.sharding import PartitionSpec as P

MESH = pl.DeviceIdType.MESH
PAIR = 2


def neg_lse(values):
    top = jnp.max(values, axis=1, keepdims=True)
    return -(top[:, 0] + jnp.log(jnp.sum(jnp.exp(values - top), axis=1)))


def plain_body(hidden, router_weight, logits, first_pot, second_pot, expert_index, loss_grad):
    experts = logits.shape[1]
    total_tokens = logits.shape[0] * lax.axis_size("dp") * lax.axis_size("mp")
    ratio = experts / total_tokens
    first_row = neg_lse(logits)
    first_soft = jnp.exp(logits + first_row[:, None])
    shifted = logits + first_pot[None, :]
    second_row = neg_lse(shifted)
    second_soft = jnp.exp(shifted + second_row[:, None])
    first_col = ratio * jnp.exp(logits + first_row[:, None] + first_pot[None, :])
    prob = jnp.exp(logits + second_row[:, None] + second_pot[None, :])
    second_col = ratio * prob
    onehot = (expert_index[:, None] == jnp.arange(experts, dtype=jnp.int32)[None, :]).astype(
        jnp.float32
    )
    direct = onehot * prob * loss_grad[:, None]
    row_direct = jnp.sum(direct, axis=1)
    second_colgrad = lax.psum(jnp.sum(direct, axis=0), ("dp", "mp"))
    second_rowgrad = row_direct - jnp.dot(
        second_col, second_colgrad, precision=lax.Precision.HIGHEST
    )
    first_colgrad = lax.psum(-jnp.sum(second_rowgrad[:, None] * second_soft, axis=0), ("dp", "mp"))
    first_rowgrad = -jnp.dot(first_col, first_colgrad, precision=lax.Precision.HIGHEST)
    score_grad = (
        direct
        - second_colgrad[None, :] * second_col
        - second_rowgrad[:, None] * second_soft
        - first_colgrad[None, :] * first_col
        - first_rowgrad[:, None] * first_soft
    ).astype(jnp.bfloat16)
    score_full = lax.all_gather(score_grad, "mp", axis=0, tiled=True)
    hidden_grad = lax.dot_general(
        score_full,
        lax.all_gather(router_weight, "dp", axis=0, tiled=True),
        (((1,), (1,)), ((), ())),
        preferred_element_type=jnp.float32,
    ).astype(jnp.bfloat16)
    weight_grad = lax.psum_scatter(
        lax.dot_general(
            hidden, score_full, (((0,), (0,)), ((), ())), preferred_element_type=jnp.float32
        ),
        "dp",
        scatter_dimension=0,
        tiled=True,
    )
    return (weight_grad, hidden_grad)


def column_groups(rows, outer):
    for group in range(1, outer + 1):
        if outer % group == 0 and (group * PAIR * rows) % 128 == 0:
            return group
    return None


def kernel(
    devices_dp, devices_mp, ratio,
    hidden_hbm, w_ref, logits_ref, first_ref, second_ref, index_ref, grad_ref,
    wgrad_ref, score_ref, wfull_ref,
    hid, part, sums, ysend, yrecv, zsend, zrecv,
    hid_sem, w_send, w_recv, sum_send, sum_recv, score_send, score_recv,
    y_send, y_recv, z_send, z_recv,
):
    outer = devices_dp // PAIR
    total = devices_dp * devices_mp
    rows = w_ref.shape[0]
    tokens, experts = logits_ref.shape
    i, m = lax.axis_index("dp"), lax.axis_index("mp")
    me = i * devices_mp + m
    z, y = i // PAIR, i % PAIR
    peer = z * PAIR + 1 - y

    barrier = pltpu.get_barrier_semaphore()

    @pl.loop(1, total)
    def _(d):
        t = (me + d) % total
        pl.semaphore_signal(
            barrier, inc=1, device_id=(t // devices_mp, t % devices_mp), device_id_type=MESH
        )

    hid_copy = pltpu.make_async_copy(hidden_hbm, hid, hid_sem)
    hid_copy.start()

    first_exp = jnp.exp(first_ref[...])
    second_exp = jnp.exp(second_ref[...] - first_ref[...])
    logits = logits_ref[...]
    e = jnp.exp(logits - jnp.max(logits, axis=1, keepdims=True))
    q = e * first_exp
    first_soft = e / jnp.sum(e, axis=1, keepdims=True)
    second_soft = q / jnp.sum(q, axis=1, keepdims=True)
    chosen = lax.broadcasted_iota(jnp.int32, (tokens, experts), 1) == index_ref[...]
    direct = jnp.where(chosen, second_soft * second_exp * grad_ref[...], 0.0)
    row_direct = jnp.sum(direct, axis=1, keepdims=True)
    wfull_ref[i] = w_ref[...]

    def sum_copy(slot, t, src):
        return pltpu.make_async_remote_copy(
            src_ref=sums.at[slot, me],
            dst_ref=sums.at[slot, src],
            send_sem=sum_send.at[slot, t],
            recv_sem=sum_recv.at[slot, src],
            device_id=(t // devices_mp, t % devices_mp),
            device_id_type=MESH,
        )

    def start_sum(slot, value):
        sums[slot, me] = value

        @pl.loop(1, total)
        def _(d):
            sum_copy(slot, (me + d) % total, me).start()

    def finish_sum(slot):
        @pl.loop(1, total)
        def _(d):
            t = (me + d) % total
            sum_copy(slot, t, t).wait_recv()

        return jnp.sum(sums[slot], axis=0)

    def w_copy(way, c, target, own=False):
        return pltpu.make_async_remote_copy(
            src_ref=w_ref if own else wfull_ref.at[c],
            dst_ref=wfull_ref.at[c],
            send_sem=w_send.at[way, c],
            recv_sem=w_recv.at[c],
            device_id=(target, m),
            device_id_type=MESH,
        )

    def w_moves(step, act):
        low, high = z - step, z + step
        own = step == 0

        @pl.when((low >= 0) & (z + 1 < outer))
        def _():
            act(w_copy(0, low * PAIR + y, i + PAIR, own))

        @pl.when((high < outer) & (z >= 1))
        def _():
            act(w_copy(1, high * PAIR + y, i - PAIR, own))

        @pl.when(low >= 0)
        def _():
            act(w_copy(2, low * PAIR + y, peer, own))

        if step:

            @pl.when(high < outer)
            def _():
                act(w_copy(2, high * PAIR + y, peer))

    def w_stage(step):
        if step:

            @pl.when(z - step >= 0)
            def _():
                w_copy(0, (z - step) * PAIR + y, peer).wait_recv()

            @pl.when(z + step < outer)
            def _():
                w_copy(1, (z + step) * PAIR + y, peer).wait_recv()

        w_moves(step, lambda copy: copy.start())

    pl.semaphore_wait(barrier, total - 1)
    start_sum(0, jnp.sum(direct, axis=0, keepdims=True))
    w_stage(0)
    second_colgrad = finish_sum(0)
    second_term = (ratio * second_exp) * second_colgrad
    second_rowgrad = row_direct - jnp.sum(second_soft * second_term, axis=1, keepdims=True)
    start_sum(1, -jnp.sum(second_rowgrad * second_soft, axis=0, keepdims=True))
    if outer > 1:
        w_stage(1)
    rest = direct - second_soft * (second_term + second_rowgrad)
    first_colgrad = finish_sum(1)
    first_term = (ratio * first_exp) * first_colgrad
    first_rowgrad = -jnp.sum(first_soft * first_term, axis=1, keepdims=True)
    score_ref[m] = (rest - first_soft * (first_term + first_rowgrad)).astype(jnp.bfloat16)

    def score_copy(t, src):
        return pltpu.make_async_remote_copy(
            src_ref=score_ref.at[m],
            dst_ref=score_ref.at[src],
            send_sem=score_send.at[t],
            recv_sem=score_recv.at[src],
            device_id=(i, t),
            device_id_type=MESH,
        )

    for d in range(1, devices_mp):
        score_copy((m + d) % devices_mp, m).start()
    for step in range(2, outer):
        w_stage(step)
    hid_copy.wait()
    for d in range(1, devices_mp):
        t = (m + d) % devices_mp
        score_copy(t, t).wait_recv()

    score = score_ref[...].reshape(devices_mp * tokens, experts)
    group = column_groups(rows, outer)
    groups = outer // group
    wide = group * PAIR * rows

    def y_copy(c):
        return pltpu.make_async_remote_copy(
            src_ref=ysend.at[c],
            dst_ref=yrecv.at[c],
            send_sem=y_send.at[c],
            recv_sem=y_recv.at[c],
            device_id=(peer, m),
            device_id_type=MESH,
        )

    def z_copy(c, src):
        return pltpu.make_async_remote_copy(
            src_ref=zsend.at[c],
            dst_ref=zrecv.at[src],
            send_sem=z_send.at[c],
            recv_sem=z_recv.at[src],
            device_id=(c * PAIR + y, m),
            device_id_type=MESH,
        )

    def block(c, half):
        return pl.ds(pl.multiple_of((c * PAIR + half) * rows, 16), rows)

    order = [((z // group + 1 + k) % groups) for k in range(groups)]
    for g in order:
        columns = pl.ds(pl.multiple_of(g * wide, 128), wide)
        part[pl.ds(pl.multiple_of(g * wide, 16), wide), :] = lax.dot_general(
            hid[:, columns], score, (((0,), (0,)), ((), ())), preferred_element_type=jnp.float32
        )
        for k in range(group):
            c = g * group + k
            ysend[c] = part[block(c, 1 - y), :].astype(jnp.bfloat16)
            y_copy(c).start()

    for g in order:
        for k in range(group):
            c = g * group + k
            y_copy(c).wait_recv()
            both = part[block(c, y), :] + yrecv[c].astype(jnp.float32)

            @pl.when(c == z)
            def _():
                wgrad_ref[...] = both

            @pl.when(c != z)
            def _():
                zsend[c] = both.astype(jnp.bfloat16)
                z_copy(c, z).start()

    for c in range(outer):

        @pl.when(c != z)
        def _():
            z_copy(c, c).wait_recv()
            wgrad_ref[...] += zrecv[c].astype(jnp.float32)

    for c in range(outer):
        w_copy(2, c * PAIR + 1 - y, peer).wait_recv()

    @pl.loop(1, total)
    def _(d):
        t = (me + d) % total
        sum_copy(0, t, me).wait_send()
        sum_copy(1, t, me).wait_send()

    for step in range(outer):
        w_moves(step, lambda copy: copy.wait_send())
    for d in range(1, devices_mp):
        score_copy((m + d) % devices_mp, m).wait_send()
    for c in range(outer):
        y_copy(c).wait_send()

        @pl.when(c != z)
        def _():
            z_copy(c, z).wait_send()


def kernel_body(hidden, router_weight, logits, first_pot, second_pot, expert_index, loss_grad):
    dp, mp = lax.axis_size("dp"), lax.axis_size("mp")
    tokens, experts = logits.shape
    rows = router_weight.shape[0]
    outer = dp // PAIR
    vmem = pl.BlockSpec(memory_space=pltpu.VMEM)
    dma = pltpu.SemaphoreType.DMA
    weight_grad, score, weights = pl.pallas_call(
        functools.partial(kernel, dp, mp, experts / (tokens * dp * mp)),
        out_shape=(
            jax.ShapeDtypeStruct((rows, experts), jnp.float32),
            jax.ShapeDtypeStruct((mp, tokens, experts), jnp.bfloat16),
            jax.ShapeDtypeStruct((dp, rows, experts), jnp.bfloat16),
        ),
        in_specs=[pl.BlockSpec(memory_space=pl.ANY)] + [vmem] * 6,
        out_specs=(vmem, vmem, vmem),
        scratch_shapes=[
            pltpu.VMEM(hidden.shape, hidden.dtype),
            pltpu.VMEM((dp * rows, experts), jnp.float32),
            pltpu.VMEM((2, dp * mp, 1, experts), jnp.float32),
            pltpu.VMEM((outer, rows, experts), jnp.bfloat16),
            pltpu.VMEM((outer, rows, experts), jnp.bfloat16),
            pltpu.VMEM((outer, rows, experts), jnp.bfloat16),
            pltpu.VMEM((outer, rows, experts), jnp.bfloat16),
            dma,
            dma((3, dp)),
            dma((dp,)),
            dma((2, dp * mp)),
            dma((2, dp * mp)),
            dma((mp,)),
            dma((mp,)),
            dma((outer,)),
            dma((outer,)),
            dma((outer,)),
            dma((outer,)),
        ],
        compiler_params=pltpu.CompilerParams(
            collective_id=0, has_side_effects=True, vmem_limit_bytes=40 * 1024 * 1024
        ),
    )(
        hidden,
        router_weight,
        logits,
        first_pot[None, :],
        second_pot[None, :],
        expert_index[:, None],
        loss_grad[:, None],
    )
    hidden_grad = lax.dot_general(
        score.reshape(mp * tokens, experts),
        weights.reshape(dp * rows, experts),
        (((1,), (1,)), ((), ())),
        preferred_element_type=jnp.float32,
    ).astype(jnp.bfloat16)
    return (weight_grad, hidden_grad)


def body(hidden, router_weight, logits, *others):
    dp = lax.axis_size("dp")
    rows, tokens = router_weight.shape[0], logits.shape[0]
    fits = dp % PAIR == 0 and rows % 16 == 0 and tokens % 16 == 0
    if fits and column_groups(rows, dp // PAIR) is not None:
        return kernel_body(hidden, router_weight, logits, *others)
    return plain_body(hidden, router_weight, logits, *others)


def solution(mesh):
    in_specs = (
        P("dp", "mp"),
        P(("mp", "dp"), None),
        P(("dp", "mp"), None),
        P(),
        P(),
        P(("dp", "mp")),
        P(("dp", "mp")),
    )
    out_specs = (P(("mp", "dp"), None), P("dp", "mp"))
    return jax.shard_map(body, mesh=mesh, in_specs=in_specs, out_specs=out_specs, check_vma=False)
```

```python
import functools

import jax
import jax.numpy as jnp
from jax import lax
from jax.experimental import pallas as pl
from jax.experimental.pallas import tpu as pltpu
from jax.sharding import PartitionSpec as P

MESH = pl.DeviceIdType.MESH
BITS = [1 << k for k in range(12)]
PAIR = 2


def neg_lse(values):
    top = jnp.max(values, axis=1, keepdims=True)
    return -(top[:, 0] + jnp.log(jnp.sum(jnp.exp(values - top), axis=1)))


def plain_body(hidden, router_weight, logits, first_pot, second_pot, expert_index, loss_grad):
    experts = logits.shape[1]
    total_tokens = logits.shape[0] * lax.axis_size("dp") * lax.axis_size("mp")
    ratio = experts / total_tokens
    first_row = neg_lse(logits)
    first_soft = jnp.exp(logits + first_row[:, None])
    shifted = logits + first_pot[None, :]
    second_row = neg_lse(shifted)
    second_soft = jnp.exp(shifted + second_row[:, None])
    first_col = ratio * jnp.exp(logits + first_row[:, None] + first_pot[None, :])
    prob = jnp.exp(logits + second_row[:, None] + second_pot[None, :])
    second_col = ratio * prob
    onehot = (expert_index[:, None] == jnp.arange(experts, dtype=jnp.int32)[None, :]).astype(
        jnp.float32
    )
    direct = onehot * prob * loss_grad[:, None]
    row_direct = jnp.sum(direct, axis=1)
    second_colgrad = lax.psum(jnp.sum(direct, axis=0), ("dp", "mp"))
    second_rowgrad = row_direct - jnp.dot(
        second_col, second_colgrad, precision=lax.Precision.HIGHEST
    )
    first_colgrad = lax.psum(-jnp.sum(second_rowgrad[:, None] * second_soft, axis=0), ("dp", "mp"))
    first_rowgrad = -jnp.dot(first_col, first_colgrad, precision=lax.Precision.HIGHEST)
    score_grad = (
        direct
        - second_colgrad[None, :] * second_col
        - second_rowgrad[:, None] * second_soft
        - first_colgrad[None, :] * first_col
        - first_rowgrad[:, None] * first_soft
    ).astype(jnp.bfloat16)
    score_full = lax.all_gather(score_grad, "mp", axis=0, tiled=True)
    hidden_grad = lax.dot_general(
        score_full,
        lax.all_gather(router_weight, "dp", axis=0, tiled=True),
        (((1,), (1,)), ((), ())),
        preferred_element_type=jnp.float32,
    ).astype(jnp.bfloat16)
    weight_grad = lax.psum_scatter(
        lax.dot_general(
            hidden, score_full, (((0,), (0,)), ((), ())), preferred_element_type=jnp.float32
        ),
        "dp",
        scatter_dimension=0,
        tiled=True,
    )
    return (weight_grad, hidden_grad)


def kernel(
    devices_dp, devices_mp, ratio,
    hidden_hbm, w_ref, logits_ref, first_ref, second_ref, index_ref, grad_ref,
    wgrad_ref, score_ref, wfull_ref,
    hid, turned, logits, index, grad, pots, soft, part, sums, ysend, yrecv, zsend, zrecv,
    in_sem, w_send, w_recv, sum_send, sum_recv, row_send, row_recv,
    y_send, y_recv, z_send, z_recv,
):
    outer = devices_dp // PAIR
    total = devices_dp * devices_mp
    rows = w_ref.shape[0]
    tokens, experts = logits_ref.shape
    half = devices_mp // PAIR
    i, m = lax.axis_index("dp"), lax.axis_index("mp")
    me = i * devices_mp + m
    z, y = i // PAIR, i % PAIR
    peer = z * PAIR + 1 - y

    barrier = pltpu.get_barrier_semaphore()

    @pl.loop(1, total)
    def _(d):
        t = (me + d) % total
        pl.semaphore_signal(
            barrier, inc=1, device_id=(t // devices_mp, t % devices_mp), device_id_type=MESH
        )

    inputs = [
        (logits_ref, logits.at[m]),
        (index_ref, index.at[m]),
        (grad_ref, grad.at[m]),
        (first_ref, pots.at[0]),
        (second_ref, pots.at[1]),
        (w_ref, wfull_ref.at[i]),
        (hidden_hbm, hid),
    ]
    loads = [pltpu.make_async_copy(src, dst, in_sem.at[k]) for k, (src, dst) in enumerate(inputs)]
    for load in loads:
        load.start()
    for load in loads[:-1]:
        load.wait()

    first_exp = jnp.exp(pots[0])
    second_exp = jnp.exp(pots[1] - pots[0])

    def soften(b):
        scores = logits[b]
        e = jnp.exp(scores - jnp.max(scores, axis=1, keepdims=True))
        q = e * first_exp
        second_soft = q / jnp.sum(q, axis=1, keepdims=True)
        chosen = lax.broadcasted_iota(jnp.int32, (tokens, experts), 1) == index[b].T
        soft[0, b] = e / jnp.sum(e, axis=1, keepdims=True)
        soft[1, b] = second_soft
        soft[2, b] = jnp.where(chosen, second_soft * second_exp * grad[b].T, 0.0)

    def row_copy(kind, src, t):
        ref = (logits, index, grad)[kind]
        return pltpu.make_async_remote_copy(
            src_ref=ref.at[src],
            dst_ref=ref.at[src],
            send_sem=row_send.at[kind, src, t],
            recv_sem=row_recv.at[kind, src],
            device_id=(i, t),
            device_id_type=MESH,
        )

    beside = (m // PAIR) * PAIR + 1 - m % PAIR
    same = [(m + PAIR * d) % devices_mp for d in range(1, half)]

    soften(m)
    direct = soft[2, m]
    row_direct = jnp.sum(direct, axis=1, keepdims=True)

    def sum_copy(slot, t, src):
        return pltpu.make_async_remote_copy(
            src_ref=sums.at[slot, me],
            dst_ref=sums.at[slot, src],
            send_sem=sum_send.at[slot, t],
            recv_sem=sum_recv.at[slot, src],
            device_id=(t // devices_mp, t % devices_mp),
            device_id_type=MESH,
        )

    def start_sum(slot, value):
        sums[slot, me] = value

        @pl.loop(1, total)
        def _(d):
            sum_copy(slot, (me + d) % total, me).start()

    def finish_sum(slot):
        @pl.loop(1, total)
        def _(d):
            t = (me + d) % total
            sum_copy(slot, t, t).wait_recv()

        return jnp.sum(sums[slot], axis=0)

    def w_copy(way, c, target):
        return pltpu.make_async_remote_copy(
            src_ref=wfull_ref.at[c],
            dst_ref=wfull_ref.at[c],
            send_sem=w_send.at[way, c],
            recv_sem=w_recv.at[c],
            device_id=(target, m),
            device_id_type=MESH,
        )

    def w_along(step, act):
        low, high = z - step, z + step

        @pl.when((low >= 0) & (z + 1 < outer))
        def _():
            act(w_copy(0, low * PAIR + y, i + PAIR))

        @pl.when((high < outer) & (z >= 1))
        def _():
            act(w_copy(1, high * PAIR + y, i - PAIR))

    def w_across(step, act):
        low, high = z - step, z + step

        @pl.when(low >= 0)
        def _():
            act(w_copy(2, low * PAIR + y, peer))

        if step:

            @pl.when(high < outer)
            def _():
                act(w_copy(2, high * PAIR + y, peer))

    def w_stage(step):
        if step:

            @pl.when(z - step >= 0)
            def _():
                w_copy(0, (z - step) * PAIR + y, peer).wait_recv()

            @pl.when(z + step < outer)
            def _():
                w_copy(1, (z + step) * PAIR + y, peer).wait_recv()

        w_along(step, lambda copy: copy.start())
        w_across(step, lambda copy: copy.start())

    pl.semaphore_wait(barrier, total - 1)
    start_sum(0, jnp.sum(direct, axis=0, keepdims=True))
    for t in [beside] + same:
        for kind in range(3):
            row_copy(kind, m, t).start()
    w_stage(0)
    loads[-1].wait()
    cut = hid.shape[1] // 2
    turned[:cut, :] = hid[:, :cut].T
    second_colgrad = finish_sum(0)
    second_term = (ratio * second_exp) * second_colgrad
    second_soft = soft[1, m]
    second_rowgrad = row_direct - jnp.sum(second_soft * second_term, axis=1, keepdims=True)
    start_sum(1, -jnp.sum(second_rowgrad * second_soft, axis=0, keepdims=True))
    for t in same:
        for kind in range(3):
            row_copy(kind, t, beside).wait_recv()
            row_copy(kind, t, beside).start()
    if outer > 1:
        w_stage(1)
    turned[cut:, :] = hid[:, cut:].T
    for t in same:
        soften(t)
    for t in [beside] + [(t // PAIR) * PAIR + 1 - t % PAIR for t in same]:
        for kind in range(3):
            row_copy(kind, t, beside).wait_recv()
        soften(t)
    first_colgrad = finish_sum(1)
    first_term = (ratio * first_exp) * first_colgrad
    for b in range(devices_mp):
        first_soft, second_soft, direct = soft[0, b], soft[1, b], soft[2, b]
        second_rowgrad = jnp.sum(direct - second_soft * second_term, axis=1, keepdims=True)
        first_rowgrad = -jnp.sum(first_soft * first_term, axis=1, keepdims=True)
        score_ref[b] = (
            direct
            - second_soft * (second_term + second_rowgrad)
            - first_soft * (first_term + first_rowgrad)
        ).astype(jnp.bfloat16)

    score = score_ref[...].reshape(devices_mp * tokens, experts)

    def y_copy(c):
        return pltpu.make_async_remote_copy(
            src_ref=ysend.at[c],
            dst_ref=yrecv.at[c],
            send_sem=y_send.at[c],
            recv_sem=y_recv.at[c],
            device_id=(peer, m),
            device_id_type=MESH,
        )

    def z_copy(c, src):
        return pltpu.make_async_remote_copy(
            src_ref=zsend.at[c],
            dst_ref=zrecv.at[src],
            send_sem=z_send.at[c],
            recv_sem=z_recv.at[src],
            device_id=(c * PAIR + y, m),
            device_id_type=MESH,
        )

    def block(c, half):
        return pl.ds(pl.multiple_of((c * PAIR + half) * rows, 16), rows)

    def product(c, side):
        return jnp.dot(turned[block(c, side), :], score, preferred_element_type=jnp.float32)

    if outer & (outer - 1) == 0:
        order = [z + sum(bit * (1 - 2 * (z // bit % 2)) for bit in BITS if flip & bit) for flip in range(outer - 1, -1, -1)]
    else:
        order = [(z + 1 + k) % outer for k in range(outer)]
    for c in order:
        ysend[c] = product(c, 1 - y).astype(jnp.bfloat16)
        y_copy(c).start()
    for step in range(2, outer - 1):
        w_stage(step)
    for c in order:
        part[c] = product(c, y)
    for c in order[:-1]:
        y_copy(c).wait_recv()
        zsend[c] = (part[c] + yrecv[c].astype(jnp.float32)).astype(jnp.bfloat16)
        z_copy(c, z).start()
    if outer > 2:
        w_stage(outer - 1)
    y_copy(z).wait_recv()
    wgrad_ref[...] = part[z] + yrecv[z].astype(jnp.float32)

    for c in range(outer):

        @pl.when(c != z)
        def _():
            z_copy(c, c).wait_recv()
            wgrad_ref[...] += zrecv[c].astype(jnp.float32)

    for c in range(outer):
        w_copy(2, c * PAIR + 1 - y, peer).wait_recv()

    @pl.loop(1, total)
    def _(d):
        t = (me + d) % total
        sum_copy(0, t, me).wait_send()
        sum_copy(1, t, me).wait_send()

    for step in range(outer):
        w_along(step, lambda copy: copy.wait_send())
        w_across(step, lambda copy: copy.wait_send())
    for kind in range(3):
        for t in [beside] + same:
            row_copy(kind, m, t).wait_send()
        for t in same:
            row_copy(kind, t, beside).wait_send()
    for c in range(outer):
        y_copy(c).wait_send()

        @pl.when(c != z)
        def _():
            z_copy(c, z).wait_send()


def kernel_body(hidden, router_weight, logits, first_pot, second_pot, expert_index, loss_grad):
    dp, mp = lax.axis_size("dp"), lax.axis_size("mp")
    tokens, experts = logits.shape
    rows = router_weight.shape[0]
    outer = dp // PAIR
    vmem = pl.BlockSpec(memory_space=pltpu.VMEM)
    dma = pltpu.SemaphoreType.DMA
    weight_grad, score, weights = pl.pallas_call(
        functools.partial(kernel, dp, mp, experts / (tokens * dp * mp)),
        out_shape=(
            jax.ShapeDtypeStruct((rows, experts), jnp.float32),
            jax.ShapeDtypeStruct((mp, tokens, experts), jnp.bfloat16),
            jax.ShapeDtypeStruct((dp, rows, experts), jnp.bfloat16),
        ),
        in_specs=[pl.BlockSpec(memory_space=pltpu.HBM)] * 7,
        out_specs=(vmem, vmem, vmem),
        scratch_shapes=[
            pltpu.VMEM(hidden.shape, hidden.dtype),
            pltpu.VMEM(hidden.shape[::-1], hidden.dtype),
            pltpu.VMEM((mp, tokens, experts), jnp.float32),
            pltpu.VMEM((mp, 1, tokens), jnp.int32),
            pltpu.VMEM((mp, 1, tokens), jnp.float32),
            pltpu.VMEM((2, 1, experts), jnp.float32),
            pltpu.VMEM((3, mp, tokens, experts), jnp.float32),
            pltpu.VMEM((outer, rows, experts), jnp.float32),
            pltpu.VMEM((2, dp * mp, 1, experts), jnp.float32),
            pltpu.VMEM((outer, rows, experts), jnp.bfloat16),
            pltpu.VMEM((outer, rows, experts), jnp.bfloat16),
            pltpu.VMEM((outer, rows, experts), jnp.bfloat16),
            pltpu.VMEM((outer, rows, experts), jnp.bfloat16),
            dma((7,)),
            dma((3, dp)),
            dma((dp,)),
            dma((2, dp * mp)),
            dma((2, dp * mp)),
            dma((3, mp, mp)),
            dma((3, mp)),
            dma((outer,)),
            dma((outer,)),
            dma((outer,)),
            dma((outer,)),
        ],
        compiler_params=pltpu.CompilerParams(
            collective_id=0, has_side_effects=True, vmem_limit_bytes=67043328
        ),
    )(
        hidden,
        router_weight,
        logits,
        first_pot[None, :],
        second_pot[None, :],
        expert_index[None, :],
        loss_grad[None, :],
    )
    hidden_grad = lax.dot_general(
        score.reshape(mp * tokens, experts),
        weights.reshape(dp * rows, experts),
        (((1,), (1,)), ((), ())),
        preferred_element_type=jnp.float32,
    ).astype(jnp.bfloat16)
    return (weight_grad, hidden_grad)


def body(hidden, router_weight, logits, *others):
    dp = lax.axis_size("dp")
    rows, tokens = router_weight.shape[0], logits.shape[0]
    if dp % PAIR == 0 and lax.axis_size("mp") % PAIR == 0 and rows % 16 == 0 and tokens % 16 == 0:
        return kernel_body(hidden, router_weight, logits, *others)
    return plain_body(hidden, router_weight, logits, *others)


def solution(mesh):
    in_specs = (
        P("dp", "mp"),
        P(("mp", "dp"), None),
        P(("dp", "mp"), None),
        P(),
        P(),
        P(("dp", "mp")),
        P(("dp", "mp")),
    )
    out_specs = (P(("mp", "dp"), None), P("dp", "mp"))
    return jax.shard_map(body, mesh=mesh, in_specs=in_specs, out_specs=out_specs, check_vma=False)
```

```python
import functools

import jax
import jax.numpy as jnp
from jax import lax
from jax.experimental import pallas as pl
from jax.experimental.pallas import tpu as pltpu
from jax.sharding import PartitionSpec as P

MESH = pl.DeviceIdType.MESH
BITS = [1 << k for k in range(12)]
PAIR = 2


def neg_lse(values):
    top = jnp.max(values, axis=1, keepdims=True)
    return -(top[:, 0] + jnp.log(jnp.sum(jnp.exp(values - top), axis=1)))


def plain_body(hidden, router_weight, logits, first_pot, second_pot, expert_index, loss_grad):
    experts = logits.shape[1]
    total_tokens = logits.shape[0] * lax.axis_size("dp") * lax.axis_size("mp")
    ratio = experts / total_tokens
    first_row = neg_lse(logits)
    first_soft = jnp.exp(logits + first_row[:, None])
    shifted = logits + first_pot[None, :]
    second_row = neg_lse(shifted)
    second_soft = jnp.exp(shifted + second_row[:, None])
    first_col = ratio * jnp.exp(logits + first_row[:, None] + first_pot[None, :])
    prob = jnp.exp(logits + second_row[:, None] + second_pot[None, :])
    second_col = ratio * prob
    onehot = (expert_index[:, None] == jnp.arange(experts, dtype=jnp.int32)[None, :]).astype(
        jnp.float32
    )
    direct = onehot * prob * loss_grad[:, None]
    row_direct = jnp.sum(direct, axis=1)
    second_colgrad = lax.psum(jnp.sum(direct, axis=0), ("dp", "mp"))
    second_rowgrad = row_direct - jnp.dot(
        second_col, second_colgrad, precision=lax.Precision.HIGHEST
    )
    first_colgrad = lax.psum(-jnp.sum(second_rowgrad[:, None] * second_soft, axis=0), ("dp", "mp"))
    first_rowgrad = -jnp.dot(first_col, first_colgrad, precision=lax.Precision.HIGHEST)
    score_grad = (
        direct
        - second_colgrad[None, :] * second_col
        - second_rowgrad[:, None] * second_soft
        - first_colgrad[None, :] * first_col
        - first_rowgrad[:, None] * first_soft
    ).astype(jnp.bfloat16)
    score_full = lax.all_gather(score_grad, "mp", axis=0, tiled=True)
    hidden_grad = lax.dot_general(
        score_full,
        lax.all_gather(router_weight, "dp", axis=0, tiled=True),
        (((1,), (1,)), ((), ())),
        preferred_element_type=jnp.float32,
    ).astype(jnp.bfloat16)
    weight_grad = lax.psum_scatter(
        lax.dot_general(
            hidden, score_full, (((0,), (0,)), ((), ())), preferred_element_type=jnp.float32
        ),
        "dp",
        scatter_dimension=0,
        tiled=True,
    )
    return (weight_grad, hidden_grad)


def column_groups(rows, outer):
    for group in range(1, outer + 1):
        if outer % group == 0 and (group * PAIR * rows) % 128 == 0:
            return group
    return None


def kernel(
    devices_dp, devices_mp, ratio,
    hidden_hbm, w_ref, logits_ref, first_ref, second_ref, index_ref, grad_ref,
    wgrad_out, hgrad_out,
    wgrad_ref, hgrad, score_ref, wfull_ref, hid, turned, logits, index, grad, pots, soft, part, sums, ysend, yrecv, zsend, zrecv,
    in_sem, w_send, w_recv, sum_send, sum_recv, row_send, row_recv,
    y_send, y_recv, z_send, z_recv, out_sem,
):
    outer = devices_dp // PAIR
    total = devices_dp * devices_mp
    rows = w_ref.shape[0]
    tokens, experts = logits_ref.shape
    half = devices_mp // PAIR
    i, m = lax.axis_index("dp"), lax.axis_index("mp")
    me = i * devices_mp + m
    z, y = i // PAIR, i % PAIR
    peer = z * PAIR + 1 - y

    barrier = pltpu.get_barrier_semaphore()

    @pl.loop(1, total)
    def _(d):
        t = (me + d) % total
        pl.semaphore_signal(
            barrier, inc=1, device_id=(t // devices_mp, t % devices_mp), device_id_type=MESH
        )

    inputs = [
        (logits_ref, logits.at[m]),
        (index_ref, index.at[m]),
        (grad_ref, grad.at[m]),
        (first_ref, pots.at[0]),
        (second_ref, pots.at[1]),
        (w_ref, wfull_ref.at[i]),
        (hidden_hbm, hid),
    ]
    loads = [pltpu.make_async_copy(src, dst, in_sem.at[k]) for k, (src, dst) in enumerate(inputs)]
    for load in loads:
        load.start()
    for load in loads[:-1]:
        load.wait()

    first_exp = jnp.exp(pots[0])
    second_exp = jnp.exp(pots[1] - pots[0])

    def soften(b):
        scores = logits[b]
        e = jnp.exp(scores - jnp.max(scores, axis=1, keepdims=True))
        q = e * first_exp
        second_soft = q / jnp.sum(q, axis=1, keepdims=True)
        chosen = lax.broadcasted_iota(jnp.int32, (tokens, experts), 1) == index[b].T
        soft[0, b] = e / jnp.sum(e, axis=1, keepdims=True)
        soft[1, b] = second_soft
        soft[2, b] = jnp.where(chosen, second_soft * second_exp * grad[b].T, 0.0)

    def row_copy(kind, src, t):
        ref = (logits, index, grad)[kind]
        return pltpu.make_async_remote_copy(
            src_ref=ref.at[src],
            dst_ref=ref.at[src],
            send_sem=row_send.at[kind, src, t],
            recv_sem=row_recv.at[kind, src],
            device_id=(i, t),
            device_id_type=MESH,
        )

    beside = (m // PAIR) * PAIR + 1 - m % PAIR
    same = [(m + PAIR * d) % devices_mp for d in range(1, half)]

    soften(m)
    direct = soft[2, m]
    row_direct = jnp.sum(direct, axis=1, keepdims=True)

    def sum_copy(slot, t, src):
        return pltpu.make_async_remote_copy(
            src_ref=sums.at[slot, me],
            dst_ref=sums.at[slot, src],
            send_sem=sum_send.at[slot, t],
            recv_sem=sum_recv.at[slot, src],
            device_id=(t // devices_mp, t % devices_mp),
            device_id_type=MESH,
        )

    def start_sum(slot, value):
        sums[slot, me] = value

        @pl.loop(1, total)
        def _(d):
            sum_copy(slot, (me + d) % total, me).start()

    def finish_sum(slot):
        @pl.loop(1, total)
        def _(d):
            t = (me + d) % total
            sum_copy(slot, t, t).wait_recv()

        return jnp.sum(sums[slot], axis=0)

    def w_copy(way, c, target):
        return pltpu.make_async_remote_copy(
            src_ref=wfull_ref.at[c],
            dst_ref=wfull_ref.at[c],
            send_sem=w_send.at[way, c],
            recv_sem=w_recv.at[c],
            device_id=(target, m),
            device_id_type=MESH,
        )

    def w_along(step, act):
        low, high = z - step, z + step

        @pl.when((low >= 0) & (z + 1 < outer))
        def _():
            act(w_copy(0, low * PAIR + y, i + PAIR))

        @pl.when((high < outer) & (z >= 1))
        def _():
            act(w_copy(1, high * PAIR + y, i - PAIR))

    def w_across(step, act):
        low, high = z - step, z + step

        @pl.when(low >= 0)
        def _():
            act(w_copy(2, low * PAIR + y, peer))

        if step:

            @pl.when(high < outer)
            def _():
                act(w_copy(2, high * PAIR + y, peer))

    def w_stage(step):
        if step:

            @pl.when(z - step >= 0)
            def _():
                w_copy(0, (z - step) * PAIR + y, peer).wait_recv()

            @pl.when(z + step < outer)
            def _():
                w_copy(1, (z + step) * PAIR + y, peer).wait_recv()

        w_along(step, lambda copy: copy.start())
        w_across(step, lambda copy: copy.start())

    pl.semaphore_wait(barrier, total - 1)
    start_sum(0, jnp.sum(direct, axis=0, keepdims=True))
    for t in [beside] + same:
        for kind in range(3):
            row_copy(kind, m, t).start()
    w_stage(0)
    loads[-1].wait()
    cut = hid.shape[1] // 2
    turned[:cut, :] = hid[:, :cut].T
    second_colgrad = finish_sum(0)
    second_term = (ratio * second_exp) * second_colgrad
    second_soft = soft[1, m]
    second_rowgrad = row_direct - jnp.sum(second_soft * second_term, axis=1, keepdims=True)
    start_sum(1, -jnp.sum(second_rowgrad * second_soft, axis=0, keepdims=True))
    for t in same:
        for kind in range(3):
            row_copy(kind, t, beside).wait_recv()
            row_copy(kind, t, beside).start()
    if outer > 1:
        w_stage(1)
    turned[cut:, :] = hid[:, cut:].T
    for t in same:
        soften(t)
    for t in [beside] + [(t // PAIR) * PAIR + 1 - t % PAIR for t in same]:
        for kind in range(3):
            row_copy(kind, t, beside).wait_recv()
        soften(t)
    first_colgrad = finish_sum(1)
    first_term = (ratio * first_exp) * first_colgrad
    for b in range(devices_mp):
        first_soft, second_soft, direct = soft[0, b], soft[1, b], soft[2, b]
        second_rowgrad = jnp.sum(direct - second_soft * second_term, axis=1, keepdims=True)
        first_rowgrad = -jnp.sum(first_soft * first_term, axis=1, keepdims=True)
        score_ref[b] = (
            direct
            - second_soft * (second_term + second_rowgrad)
            - first_soft * (first_term + first_rowgrad)
        ).astype(jnp.bfloat16)

    score = score_ref[...].reshape(devices_mp * tokens, experts)

    def y_copy(c):
        return pltpu.make_async_remote_copy(
            src_ref=ysend.at[c],
            dst_ref=yrecv.at[c],
            send_sem=y_send.at[c],
            recv_sem=y_recv.at[c],
            device_id=(peer, m),
            device_id_type=MESH,
        )

    def z_copy(c, src):
        return pltpu.make_async_remote_copy(
            src_ref=zsend.at[c],
            dst_ref=zrecv.at[src],
            send_sem=z_send.at[c],
            recv_sem=z_recv.at[src],
            device_id=(c * PAIR + y, m),
            device_id_type=MESH,
        )

    def block(c, half):
        return pl.ds(pl.multiple_of((c * PAIR + half) * rows, 16), rows)

    def product(c, side):
        return jnp.dot(turned[block(c, side), :], score, preferred_element_type=jnp.float32)

    if outer & (outer - 1) == 0:
        order = [z + sum(bit * (1 - 2 * (z // bit % 2)) for bit in BITS if flip & bit) for flip in range(outer - 1, -1, -1)]
    else:
        order = [(z + 1 + k) % outer for k in range(outer)]
    for c in order:
        ysend[c] = product(c, 1 - y).astype(jnp.bfloat16)
        y_copy(c).start()
    for step in range(2, outer - 1):
        w_stage(step)
    for c in order:
        part[c] = product(c, y)

    group = column_groups(rows, outer)
    groups, wide = outer // group, group * PAIR * rows

    def hidden_out(g):
        columns = pl.ds(pl.multiple_of(g * wide, 128), wide)
        return pltpu.make_async_copy(
            hgrad.at[:, columns], hgrad_out.at[:, columns], out_sem.at[g]
        )

    def hidden_part(g):
        for k in range(group):
            w_copy(2, (g * group + k) * PAIR + 1 - y, peer).wait_recv()
        weights = wfull_ref[pl.ds(g * group * PAIR, group * PAIR)].reshape(wide, experts)
        hgrad[:, pl.ds(pl.multiple_of(g * wide, 128), wide)] = lax.dot_general(
            score, weights, (((1,), (1,)), ((), ())), preferred_element_type=jnp.float32
        ).astype(jnp.bfloat16)
        hidden_out(g).start()

    if groups > 1:
        hidden_part(z // group)
    for c in order[:-1]:
        y_copy(c).wait_recv()
        zsend[c] = (part[c] + yrecv[c].astype(jnp.float32)).astype(jnp.bfloat16)
        z_copy(c, z).start()
    if outer > 2:
        w_stage(outer - 1)
    y_copy(z).wait_recv()
    wgrad_ref[...] = part[z] + yrecv[z].astype(jnp.float32)

    for c in range(outer):

        @pl.when(c != z)
        def _():
            z_copy(c, c).wait_recv()
            wgrad_ref[...] += zrecv[c].astype(jnp.float32)

    wgrad_copy = pltpu.make_async_copy(wgrad_ref, wgrad_out, out_sem.at[groups])
    wgrad_copy.start()
    for k in range(1, groups) if groups > 1 else [0]:
        hidden_part((z // group + k) % groups)

    @pl.loop(1, total)
    def _(d):
        t = (me + d) % total
        sum_copy(0, t, me).wait_send()
        sum_copy(1, t, me).wait_send()

    for step in range(outer):
        w_along(step, lambda copy: copy.wait_send())
        w_across(step, lambda copy: copy.wait_send())
    for kind in range(3):
        for t in [beside] + same:
            row_copy(kind, m, t).wait_send()
        for t in same:
            row_copy(kind, t, beside).wait_send()
    for c in range(outer):
        y_copy(c).wait_send()

        @pl.when(c != z)
        def _():
            z_copy(c, z).wait_send()

    wgrad_copy.wait()
    for g in range(groups):
        hidden_out(g).wait()


def kernel_body(hidden, router_weight, logits, first_pot, second_pot, expert_index, loss_grad):
    dp, mp = lax.axis_size("dp"), lax.axis_size("mp")
    tokens, experts = logits.shape
    rows = router_weight.shape[0]
    outer = dp // PAIR
    hbm = pl.BlockSpec(memory_space=pltpu.HBM)
    group = column_groups(rows, outer)
    dma = pltpu.SemaphoreType.DMA
    return pl.pallas_call(
        functools.partial(kernel, dp, mp, experts / (tokens * dp * mp)),
        out_shape=(
            jax.ShapeDtypeStruct((rows, experts), jnp.float32),
            jax.ShapeDtypeStruct((mp * tokens, dp * rows), jnp.bfloat16),
        ),
        in_specs=[hbm] * 7,
        out_specs=(hbm, hbm),
        scratch_shapes=[
            pltpu.VMEM((rows, experts), jnp.float32),
            pltpu.VMEM(hidden.shape, hidden.dtype),
            pltpu.VMEM((mp, tokens, experts), jnp.bfloat16),
            pltpu.VMEM((dp, rows, experts), jnp.bfloat16),
            pltpu.VMEM(hidden.shape, hidden.dtype),
            pltpu.VMEM(hidden.shape[::-1], hidden.dtype),
            pltpu.VMEM((mp, tokens, experts), jnp.float32),
            pltpu.VMEM((mp, 1, tokens), jnp.int32),
            pltpu.VMEM((mp, 1, tokens), jnp.float32),
            pltpu.VMEM((2, 1, experts), jnp.float32),
            pltpu.VMEM((3, mp, tokens, experts), jnp.float32),
            pltpu.VMEM((outer, rows, experts), jnp.float32),
            pltpu.VMEM((2, dp * mp, 1, experts), jnp.float32),
            pltpu.VMEM((outer, rows, experts), jnp.bfloat16),
            pltpu.VMEM((outer, rows, experts), jnp.bfloat16),
            pltpu.VMEM((outer, rows, experts), jnp.bfloat16),
            pltpu.VMEM((outer, rows, experts), jnp.bfloat16),
            dma((7,)),
            dma((3, dp)),
            dma((dp,)),
            dma((2, dp * mp)),
            dma((2, dp * mp)),
            dma((3, mp, mp)),
            dma((3, mp)),
            dma((outer,)),
            dma((outer,)),
            dma((outer,)),
            dma((outer,)),
            dma((outer // group + 1,)),
        ],
        compiler_params=pltpu.CompilerParams(
            collective_id=0, has_side_effects=True, vmem_limit_bytes=67043328
        ),
    )(
        hidden,
        router_weight,
        logits,
        first_pot[None, :],
        second_pot[None, :],
        expert_index[None, :],
        loss_grad[None, :],
    )


def body(hidden, router_weight, logits, *others):
    dp = lax.axis_size("dp")
    rows, tokens = router_weight.shape[0], logits.shape[0]
    pairs = dp % PAIR == 0 and lax.axis_size("mp") % PAIR == 0
    if pairs and rows % 16 == 0 and tokens % 16 == 0 and column_groups(rows, dp // PAIR):
        return kernel_body(hidden, router_weight, logits, *others)
    return plain_body(hidden, router_weight, logits, *others)


def solution(mesh):
    in_specs = (
        P("dp", "mp"),
        P(("mp", "dp"), None),
        P(("dp", "mp"), None),
        P(),
        P(),
        P(("dp", "mp")),
        P(("dp", "mp")),
    )
    out_specs = (P(("mp", "dp"), None), P("dp", "mp"))
    return jax.shard_map(body, mesh=mesh, in_specs=in_specs, out_specs=out_specs, check_vma=False)
```

```python
import functools

import jax
import jax.numpy as jnp
from jax import lax
from jax.experimental import pallas as pl
from jax.experimental.pallas import tpu as pltpu
from jax.sharding import PartitionSpec as P

MESH = pl.DeviceIdType.MESH
BITS = [1 << k for k in range(12)]
PAIR = 2


def neg_lse(values):
    top = jnp.max(values, axis=1, keepdims=True)
    return -(top[:, 0] + jnp.log(jnp.sum(jnp.exp(values - top), axis=1)))


def plain_body(hidden, router_weight, logits, first_pot, second_pot, expert_index, loss_grad):
    experts = logits.shape[1]
    total_tokens = logits.shape[0] * lax.axis_size("dp") * lax.axis_size("mp")
    ratio = experts / total_tokens
    first_row = neg_lse(logits)
    first_soft = jnp.exp(logits + first_row[:, None])
    shifted = logits + first_pot[None, :]
    second_row = neg_lse(shifted)
    second_soft = jnp.exp(shifted + second_row[:, None])
    first_col = ratio * jnp.exp(logits + first_row[:, None] + first_pot[None, :])
    prob = jnp.exp(logits + second_row[:, None] + second_pot[None, :])
    second_col = ratio * prob
    onehot = (expert_index[:, None] == jnp.arange(experts, dtype=jnp.int32)[None, :]).astype(
        jnp.float32
    )
    direct = onehot * prob * loss_grad[:, None]
    row_direct = jnp.sum(direct, axis=1)
    second_colgrad = lax.psum(jnp.sum(direct, axis=0), ("dp", "mp"))
    second_rowgrad = row_direct - jnp.dot(
        second_col, second_colgrad, precision=lax.Precision.HIGHEST
    )
    first_colgrad = lax.psum(-jnp.sum(second_rowgrad[:, None] * second_soft, axis=0), ("dp", "mp"))
    first_rowgrad = -jnp.dot(first_col, first_colgrad, precision=lax.Precision.HIGHEST)
    score_grad = (
        direct
        - second_colgrad[None, :] * second_col
        - second_rowgrad[:, None] * second_soft
        - first_colgrad[None, :] * first_col
        - first_rowgrad[:, None] * first_soft
    ).astype(jnp.bfloat16)
    score_full = lax.all_gather(score_grad, "mp", axis=0, tiled=True)
    hidden_grad = lax.dot_general(
        score_full,
        lax.all_gather(router_weight, "dp", axis=0, tiled=True),
        (((1,), (1,)), ((), ())),
        preferred_element_type=jnp.float32,
    ).astype(jnp.bfloat16)
    weight_grad = lax.psum_scatter(
        lax.dot_general(
            hidden, score_full, (((0,), (0,)), ((), ())), preferred_element_type=jnp.float32
        ),
        "dp",
        scatter_dimension=0,
        tiled=True,
    )
    return (weight_grad, hidden_grad)


def kernel(
    devices_dp, devices_mp, ratio,
    hidden_hbm, w_ref, logits_ref, first_ref, second_ref, index_ref, grad_ref,
    wgrad_out, score_out, wfull_out,
    wgrad_ref, score_ref, wfull_ref, hid, turned, logits, index, grad, pots, soft, part, sums, ysend, yrecv, zsend, zrecv,
    in_sem, w_send, w_recv, sum_send, sum_recv, row_send, row_recv,
    y_send, y_recv, z_send, z_recv, out_sem,
):
    outer = devices_dp // PAIR
    total = devices_dp * devices_mp
    rows = w_ref.shape[0]
    tokens, experts = logits_ref.shape
    half = devices_mp // PAIR
    i, m = lax.axis_index("dp"), lax.axis_index("mp")
    me = i * devices_mp + m
    z, y = i // PAIR, i % PAIR
    peer = z * PAIR + 1 - y

    barrier = pltpu.get_barrier_semaphore()

    @pl.loop(1, total)
    def _(d):
        t = (me + d) % total
        pl.semaphore_signal(
            barrier, inc=1, device_id=(t // devices_mp, t % devices_mp), device_id_type=MESH
        )

    inputs = [
        (logits_ref, logits.at[m]),
        (index_ref, index.at[m]),
        (grad_ref, grad.at[m]),
        (first_ref, pots.at[0]),
        (second_ref, pots.at[1]),
        (w_ref, wfull_ref.at[i]),
        (hidden_hbm, hid),
    ]
    loads = [pltpu.make_async_copy(src, dst, in_sem.at[k]) for k, (src, dst) in enumerate(inputs)]
    for load in loads:
        load.start()
    for load in loads[:-1]:
        load.wait()

    first_exp = jnp.exp(pots[0])
    second_exp = jnp.exp(pots[1] - pots[0])

    def soften(b):
        scores = logits[b]
        e = jnp.exp(scores - jnp.max(scores, axis=1, keepdims=True))
        q = e * first_exp
        second_soft = q / jnp.sum(q, axis=1, keepdims=True)
        chosen = lax.broadcasted_iota(jnp.int32, (tokens, experts), 1) == index[b].T
        soft[0, b] = e / jnp.sum(e, axis=1, keepdims=True)
        soft[1, b] = second_soft
        soft[2, b] = jnp.where(chosen, second_soft * second_exp * grad[b].T, 0.0)

    def row_copy(kind, src, t):
        ref = (logits, index, grad)[kind]
        return pltpu.make_async_remote_copy(
            src_ref=ref.at[src],
            dst_ref=ref.at[src],
            send_sem=row_send.at[kind, src, t],
            recv_sem=row_recv.at[kind, src],
            device_id=(i, t),
            device_id_type=MESH,
        )

    beside = (m // PAIR) * PAIR + 1 - m % PAIR
    same = [(m + PAIR * d) % devices_mp for d in range(1, half)]

    soften(m)
    direct = soft[2, m]
    row_direct = jnp.sum(direct, axis=1, keepdims=True)

    def sum_copy(slot, t, src):
        return pltpu.make_async_remote_copy(
            src_ref=sums.at[slot, me],
            dst_ref=sums.at[slot, src],
            send_sem=sum_send.at[slot, t],
            recv_sem=sum_recv.at[slot, src],
            device_id=(t // devices_mp, t % devices_mp),
            device_id_type=MESH,
        )

    def start_sum(slot, value):
        sums[slot, me] = value

        @pl.loop(1, total)
        def _(d):
            sum_copy(slot, (me + d) % total, me).start()

    def finish_sum(slot):
        @pl.loop(1, total)
        def _(d):
            t = (me + d) % total
            sum_copy(slot, t, t).wait_recv()

        return jnp.sum(sums[slot], axis=0)

    def w_copy(way, c, target):
        return pltpu.make_async_remote_copy(
            src_ref=wfull_ref.at[c],
            dst_ref=wfull_ref.at[c],
            send_sem=w_send.at[way, c],
            recv_sem=w_recv.at[c],
            device_id=(target, m),
            device_id_type=MESH,
        )

    def w_along(step, act):
        low, high = z - step, z + step

        @pl.when((low >= 0) & (z + 1 < outer))
        def _():
            act(w_copy(0, low * PAIR + y, i + PAIR))

        @pl.when((high < outer) & (z >= 1))
        def _():
            act(w_copy(1, high * PAIR + y, i - PAIR))

    def w_across(step, act):
        low, high = z - step, z + step

        @pl.when(low >= 0)
        def _():
            act(w_copy(2, low * PAIR + y, peer))

        if step:

            @pl.when(high < outer)
            def _():
                act(w_copy(2, high * PAIR + y, peer))

    def w_stage(step):
        if step:

            @pl.when(z - step >= 0)
            def _():
                w_copy(0, (z - step) * PAIR + y, peer).wait_recv()

            @pl.when(z + step < outer)
            def _():
                w_copy(1, (z + step) * PAIR + y, peer).wait_recv()

        w_along(step, lambda copy: copy.start())
        w_across(step, lambda copy: copy.start())

    pl.semaphore_wait(barrier, total - 1)
    start_sum(0, jnp.sum(direct, axis=0, keepdims=True))
    for t in [beside] + same:
        for kind in range(3):
            row_copy(kind, m, t).start()
    w_stage(0)
    loads[-1].wait()
    cut = hid.shape[1] // 2
    turned[:cut, :] = hid[:, :cut].T
    second_colgrad = finish_sum(0)
    second_term = (ratio * second_exp) * second_colgrad
    second_soft = soft[1, m]
    second_rowgrad = row_direct - jnp.sum(second_soft * second_term, axis=1, keepdims=True)
    start_sum(1, -jnp.sum(second_rowgrad * second_soft, axis=0, keepdims=True))
    for t in same:
        for kind in range(3):
            row_copy(kind, t, beside).wait_recv()
            row_copy(kind, t, beside).start()
    if outer > 1:
        w_stage(1)
    turned[cut:, :] = hid[:, cut:].T
    for t in same:
        soften(t)
    for t in [beside] + [(t // PAIR) * PAIR + 1 - t % PAIR for t in same]:
        for kind in range(3):
            row_copy(kind, t, beside).wait_recv()
        soften(t)
    first_colgrad = finish_sum(1)
    first_term = (ratio * first_exp) * first_colgrad
    for b in range(devices_mp):
        first_soft, second_soft, direct = soft[0, b], soft[1, b], soft[2, b]
        second_rowgrad = jnp.sum(direct - second_soft * second_term, axis=1, keepdims=True)
        first_rowgrad = -jnp.sum(first_soft * first_term, axis=1, keepdims=True)
        score_ref[b] = (
            direct
            - second_soft * (second_term + second_rowgrad)
            - first_soft * (first_term + first_rowgrad)
        ).astype(jnp.bfloat16)

    score = score_ref[...].reshape(devices_mp * tokens, experts)

    def y_copy(c):
        return pltpu.make_async_remote_copy(
            src_ref=ysend.at[c],
            dst_ref=yrecv.at[c],
            send_sem=y_send.at[c],
            recv_sem=y_recv.at[c],
            device_id=(peer, m),
            device_id_type=MESH,
        )

    def z_copy(c, src):
        return pltpu.make_async_remote_copy(
            src_ref=zsend.at[c],
            dst_ref=zrecv.at[src],
            send_sem=z_send.at[c],
            recv_sem=z_recv.at[src],
            device_id=(c * PAIR + y, m),
            device_id_type=MESH,
        )

    def block(c, half):
        return pl.ds(pl.multiple_of((c * PAIR + half) * rows, 16), rows)

    def product(c, side):
        return jnp.dot(turned[block(c, side), :], score, preferred_element_type=jnp.float32)

    if outer & (outer - 1) == 0:
        order = [z + sum(bit * (1 - 2 * (z // bit % 2)) for bit in BITS if flip & bit) for flip in range(outer - 1, -1, -1)]
    else:
        order = [(z + 1 + k) % outer for k in range(outer)]
    for c in order:
        ysend[c] = product(c, 1 - y).astype(jnp.bfloat16)
        y_copy(c).start()
    for step in range(2, outer - 1):
        w_stage(step)
    for c in order:
        part[c] = product(c, y)

    group = 2 if outer % 2 == 0 else 1
    groups = outer // group
    score_copy = pltpu.make_async_copy(score_ref, score_out, out_sem.at[groups + 1])
    score_copy.start()

    def rows_out(g):
        chunks = pl.ds(g * group * PAIR, group * PAIR)
        return pltpu.make_async_copy(wfull_ref.at[chunks], wfull_out.at[chunks], out_sem.at[g])

    def rows_ready(g):
        for k in range(group):
            w_copy(2, (g * group + k) * PAIR + 1 - y, peer).wait_recv()
        rows_out(g).start()

    if groups > 1:
        rows_ready(z // group)
    for c in order[:-1]:
        y_copy(c).wait_recv()
        zsend[c] = (part[c] + yrecv[c].astype(jnp.float32)).astype(jnp.bfloat16)
        z_copy(c, z).start()
    if outer > 2:
        w_stage(outer - 1)
    y_copy(z).wait_recv()
    wgrad_ref[...] = part[z] + yrecv[z].astype(jnp.float32)

    for c in range(outer):

        @pl.when(c != z)
        def _():
            z_copy(c, c).wait_recv()
            wgrad_ref[...] += zrecv[c].astype(jnp.float32)

    wgrad_copy = pltpu.make_async_copy(wgrad_ref, wgrad_out, out_sem.at[groups])
    wgrad_copy.start()
    for k in range(1, groups) if groups > 1 else [0]:
        rows_ready((z // group + k) % groups)

    @pl.loop(1, total)
    def _(d):
        t = (me + d) % total
        sum_copy(0, t, me).wait_send()
        sum_copy(1, t, me).wait_send()

    for step in range(outer):
        w_along(step, lambda copy: copy.wait_send())
        w_across(step, lambda copy: copy.wait_send())
    for kind in range(3):
        for t in [beside] + same:
            row_copy(kind, m, t).wait_send()
        for t in same:
            row_copy(kind, t, beside).wait_send()
    for c in range(outer):
        y_copy(c).wait_send()

        @pl.when(c != z)
        def _():
            z_copy(c, z).wait_send()

    wgrad_copy.wait()
    score_copy.wait()
    for g in range(groups):
        rows_out(g).wait()


def kernel_body(hidden, router_weight, logits, first_pot, second_pot, expert_index, loss_grad):
    dp, mp = lax.axis_size("dp"), lax.axis_size("mp")
    tokens, experts = logits.shape
    rows = router_weight.shape[0]
    outer = dp // PAIR
    hbm = pl.BlockSpec(memory_space=pltpu.HBM)
    dma = pltpu.SemaphoreType.DMA
    weight_grad, score, weights = pl.pallas_call(
        functools.partial(kernel, dp, mp, experts / (tokens * dp * mp)),
        out_shape=(
            jax.ShapeDtypeStruct((rows, experts), jnp.float32),
            jax.ShapeDtypeStruct((mp, tokens, experts), jnp.bfloat16),
            jax.ShapeDtypeStruct((dp, rows, experts), jnp.bfloat16),
        ),
        in_specs=[hbm] * 7,
        out_specs=(hbm, hbm, hbm),
        scratch_shapes=[
            pltpu.VMEM((rows, experts), jnp.float32),
            pltpu.VMEM((mp, tokens, experts), jnp.bfloat16),
            pltpu.VMEM((dp, rows, experts), jnp.bfloat16),
            pltpu.VMEM(hidden.shape, hidden.dtype),
            pltpu.VMEM(hidden.shape[::-1], hidden.dtype),
            pltpu.VMEM((mp, tokens, experts), jnp.float32),
            pltpu.VMEM((mp, 1, tokens), jnp.int32),
            pltpu.VMEM((mp, 1, tokens), jnp.float32),
            pltpu.VMEM((2, 1, experts), jnp.float32),
            pltpu.VMEM((3, mp, tokens, experts), jnp.float32),
            pltpu.VMEM((outer, rows, experts), jnp.float32),
            pltpu.VMEM((2, dp * mp, 1, experts), jnp.float32),
            pltpu.VMEM((outer, rows, experts), jnp.bfloat16),
            pltpu.VMEM((outer, rows, experts), jnp.bfloat16),
            pltpu.VMEM((outer, rows, experts), jnp.bfloat16),
            pltpu.VMEM((outer, rows, experts), jnp.bfloat16),
            dma((7,)),
            dma((3, dp)),
            dma((dp,)),
            dma((2, dp * mp)),
            dma((2, dp * mp)),
            dma((3, mp, mp)),
            dma((3, mp)),
            dma((outer,)),
            dma((outer,)),
            dma((outer,)),
            dma((outer,)),
            dma((outer + 2,)),
        ],
        compiler_params=pltpu.CompilerParams(
            collective_id=0, has_side_effects=True, vmem_limit_bytes=67043328
        ),
    )(
        hidden,
        router_weight,
        logits,
        first_pot[None, :],
        second_pot[None, :],
        expert_index[None, :],
        loss_grad[None, :],
    )
    hidden_grad = lax.dot_general(
        score.reshape(mp * tokens, experts),
        weights.reshape(dp * rows, experts),
        (((1,), (1,)), ((), ())),
        preferred_element_type=jnp.float32,
    ).astype(jnp.bfloat16)
    return (weight_grad, hidden_grad)


def body(hidden, router_weight, logits, *others):
    dp = lax.axis_size("dp")
    rows, tokens = router_weight.shape[0], logits.shape[0]
    pairs = dp % PAIR == 0 and lax.axis_size("mp") % PAIR == 0
    if pairs and rows % 16 == 0 and tokens % 16 == 0:
        return kernel_body(hidden, router_weight, logits, *others)
    return plain_body(hidden, router_weight, logits, *others)


def solution(mesh):
    in_specs = (
        P("dp", "mp"),
        P(("mp", "dp"), None),
        P(("dp", "mp"), None),
        P(),
        P(),
        P(("dp", "mp")),
        P(("dp", "mp")),
    )
    out_specs = (P(("mp", "dp"), None), P("dp", "mp"))
    return jax.shard_map(body, mesh=mesh, in_specs=in_specs, out_specs=out_specs, check_vma=False)
```
